256 devices in a mesh: section: 8 (over z_lo, x), dp: 32 (over z_hi, y, core).
Axes of the slice: x: 4, y: 4, z: 8 (z_hi: 4, z_lo: 2; z = z_hi * 2 + z_lo), core: 2. Of those that a mesh axis runs over, the one named last changes fastest.
Arguments:
- activations: bfloat16 [8, 8, 1536, 5376], P('section', None, 'dp'), may hold values from -6 to 6
- loss_grads: bfloat16 [8, 1536, 5376], P(None, 'dp'), may hold values from -6 to 6
- adapter_in: bfloat16 [8, 5376, 64], P('section'), may hold values from -0.078125 to 0.078125
- adapter_out: bfloat16 [8, 64, 5376], P('section'), may hold values from -0.75 to 0.75
- first_moment: float32 [8, 32, 43008], P('section', 'dp'), may hold values from -0.4 to 0.4
- second_moment: float32 [8, 32, 43008], P('section', 'dp'), may hold values from 0.0001 to 0.01
- old_owner: int32 [8, 16], P('section'), may hold values from 0 to 31, as said below
- new_owner: int32 [8, 32], P('section'), may hold values from 0 to 31, each once within a row
- plan: int32 [8], replicated, may hold values from 0 to 7, each once
Outputs:
- input_grads: bfloat16 [8, 8, 1536, 5376], P('section', None, 'dp')
- adam_update: float32 [8, 32, 21504], P('section', 'dp')
- first_new: float32 [8, 32, 21504], P('section', 'dp')
- second_new: float32 [8, 32, 21504], P('section', 'dp')
The draws below stay inside these ranges and needn't reach their ends.
Inputs may be any that keep to these rules, and one draw needn't show every extreme that they name: `old_owner`: the entries of one section's row are distinct.
All inputs are finite; a program needn't handle non-finite values.
Results may differ from the reference program's by a relative error of at most 0.025.
Values may be sent and summed in bfloat16 or wider, within the bound.
No kernel may reach another device: no remote copies, remote signals or barrier semaphores. Data moves between devices by JAX's collectives and lax.ppermute only.
A program may use at most 64 MiB of HBM per device.

```python
import math
import jax
import jax.numpy as jnp

D = 5376
RANK = 64
MB = 8
SECTIONS = 8
TOKENS = 1536
BLOCK = 21504
OLD_DP = 16
N_DP = 32


def draw_old_owner(key, part):
    section_keys = jax.random.split(key, SECTIONS)
    rows = jax.vmap(lambda section_key: jax.random.permutation(section_key, N_DP)[:OLD_DP])(section_keys)
    return rows.astype(jnp.int32)


def strengthened(drawn, key, source, target, parts, factor):
    owner, partner = [(jnp.arange(drawn.shape[axis_at]) // (drawn.shape[axis_at] // parts)).reshape([-1 if axis == axis_at else 1 for axis in range(drawn.ndim)]) for axis_at in (source, target)]
    chosen = jax.random.permutation(key, parts)[partner]
    strong = (owner == chosen) | (owner == (partner + parts // 2) % parts)
    return jnp.where(strong, factor * drawn, drawn)


def levels(key, shape, cuts, low, largest):
    loudness, own = 1.0, jax.random.fold_in(key, 6)
    for dim, blocks in cuts:
        steps = jnp.exp(jax.random.uniform(jax.random.fold_in(own, dim), (blocks,), jnp.float32, low / len(cuts), largest / len(cuts)))
        loudness = loudness * jnp.repeat(steps, shape[dim] // blocks).reshape([-1 if axis == dim else 1 for axis in range(len(shape))])
    return loudness


def bell_draw(stream_key, shape, width, bound, cuts=(), kind=jnp.bfloat16):
    array = jax.random.normal(stream_key, shape, jnp.float32) * width
    if len(cuts) > 0:
        array = levels(stream_key, shape, cuts, -0.22, 0.18) * array
    return jnp.clip(array, min=-bound, max=bound).astype(kind)


def heavy_noise(rng, dims, width, reach, shards, heavy, kind=jnp.bfloat16):
    array = width * jax.random.normal(rng, dims, jnp.float32)
    if shards:
        array = array * levels(rng, dims, shards, -0.22, 0.18)
    return jnp.clip(strengthened(array, jax.random.fold_in(rng, 3), *heavy), -reach, reach).astype(kind)


def setup_inputs(seed: int = 0) -> dict:
    key_of = jax.random.split(jax.random.key(seed), 10)
    activations = bell_draw(key_of[0], (SECTIONS, MB, TOKENS, D), 1.0, 6.0, ((0, 8), (2, 32)))
    loss_grads = heavy_noise(key_of[1], (MB, TOKENS, D), 1.0, 6.0, ((1, 32),), (1, 2, 32, 2.75))
    adapter_in = bell_draw(key_of[2], (SECTIONS, D, RANK), D ** -0.5, 0.078125, ((0, 8),))
    adapter_out = bell_draw(key_of[3], (SECTIONS, RANK, D), RANK ** -0.5, 0.75, ((0, 8),))
    first_moment = bell_draw(key_of[4], (SECTIONS, N_DP, 2 * BLOCK), 0.05, 0.4, ((0, 8), (1, 32)), jnp.float32)
    second_moment = jnp.clip(jnp.exp(math.log(0.01) - 4.6051702 * jax.random.uniform(key_of[5], (SECTIONS, N_DP, 2 * BLOCK), jnp.float32) ** levels(key_of[5], (SECTIONS, N_DP, 2 * BLOCK), ((0, 8), (1, 32)), -0.2, 0.2)), 0.0001, 0.01)
    old_owner = draw_old_owner(jax.random.fold_in(key_of[9], 71), 0)
    new_owner = jax.vmap(lambda own: jax.random.permutation(own, N_DP))(jax.random.split(key_of[7], SECTIONS)).reshape((SECTIONS, N_DP)).astype(jnp.int32)
    plan = jax.random.permutation(key_of[8], MB).astype(jnp.int32)
    return dict(activations=activations, loss_grads=loss_grads, adapter_in=adapter_in, adapter_out=adapter_out, first_moment=first_moment, second_moment=second_moment, old_owner=old_owner, new_owner=new_owner, plan=plan)


beta_one = 0.9
beta_two = 0.95
adam_eps = 1e-08
adam_step = 1000.0
loss_scale = 4096.0

def silu_slope(pre_value):
    gate_value = jax.nn.sigmoid(pre_value)
    return gate_value * (1.0 + pre_value * (1.0 - gate_value))

def adam_rows(grads, first, second):
    first_next = beta_one * first + (1.0 - beta_one) * grads
    second_next = beta_two * second + (1.0 - beta_two) * grads * grads
    update = first_next / (1.0 - beta_one ** adam_step) / (jnp.sqrt(second_next / (1.0 - beta_two ** adam_step)) + adam_eps)
    return (update, first_next, second_next)

def reference(activations, loss_grads, adapter_in, adapter_out, first_moment, second_moment, old_owner, new_owner, plan):
    incoming = loss_grads[plan]
    emitted = []
    updates = []
    firsts = []
    seconds = []
    for section_index in reversed(range(SECTIONS)):
        section_input = activations[section_index][plan].reshape(-1, D)
        incoming_flat = incoming.reshape(-1, D)
        weight_in = adapter_in[section_index]
        weight_out = adapter_out[section_index]
        pre_value = jnp.dot(section_input, weight_in, preferred_element_type=jnp.float32)
        hidden = jax.nn.silu(pre_value).astype(jnp.bfloat16)
        act_grad = jnp.dot(incoming_flat, weight_out.T, preferred_element_type=jnp.float32)
        pre_grad = (act_grad * silu_slope(pre_value)).astype(jnp.bfloat16)
        input_grad = (incoming_flat.astype(jnp.float32) + jnp.dot(pre_grad, weight_in.T, preferred_element_type=jnp.float32)).astype(jnp.bfloat16)
        grad_in = jnp.dot(section_input.T, pre_grad, preferred_element_type=jnp.float32)
        grad_out = jnp.dot(hidden.T, incoming_flat, preferred_element_type=jnp.float32)
        grads = jnp.concatenate([grad_in.reshape(-1), grad_out.reshape(-1)]) / loss_scale
        first_old = first_moment[section_index][old_owner[section_index]].reshape(-1)
        second_old = second_moment[section_index][old_owner[section_index]].reshape(-1)
        update, first_next, second_next = adam_rows(grads, first_old, second_old)
        inverse = jnp.argsort(new_owner[section_index]).astype(jnp.int32)
        updates.insert(0, update.reshape(N_DP, BLOCK)[inverse])
        firsts.insert(0, first_next.reshape(N_DP, BLOCK)[inverse])
        seconds.insert(0, second_next.reshape(N_DP, BLOCK)[inverse])
        incoming = input_grad.reshape(MB, TOKENS, D)
        emitted.insert(0, incoming)
    return (jnp.stack(emitted), jnp.stack(updates), jnp.stack(firsts), jnp.stack(seconds))
```

```python
import functools

import jax
import jax.numpy as jnp
from jax import lax
from jax.experimental import pallas as pl
from jax.experimental.pallas import tpu as pltpu
from jax.sharding import Mesh
from jax.sharding import PartitionSpec as P

DP = ("dp_0", "dp_1", "dp_2")

beta_one = 0.9
beta_two = 0.95
adam_eps = 1e-08
adam_step = 1000.0
loss_scale = 4096.0

LANES = 128
BF = jnp.bfloat16
F32 = jnp.float32
PIECE_ROWS = 6
HELD = (
    (0, 3, 1, 2, 6, 7, 5),
    (0, 3, 5, 2, 6, 7, -1),
    (0, 8, 5, 2, 4, -1, -1),
    (4, 8, 5, 2, -1, -1, -1),
    (0, 3, 1, -1, -1, -1, -1),
    (0, 3, -1, -1, -1, -1, -1),
    (0, -1, -1, -1, -1, -1, -1),
    (-1, -1, -1, -1, -1, -1, -1),
)


def send(value, pairs, axis="section"):
    return lax.ppermute(value, axis, pairs)


def gather_later(own):
    down = send(own, [(s, s - 1) for s in (1, 2, 3, 5, 6, 7)])
    wrap = send(own, [(3, 0), (7, 4)])
    level = send(own, [(s, s - 4) for s in (4, 5, 6, 7)])
    down_a = send(down, [(1, 0), (2, 1), (5, 4), (6, 5)])
    down_b = send(level, [(3, 2), (0, 3)])
    up = send(level, [(0, 1), (1, 2), (2, 3), (3, 0)])
    level_2 = send(down, [(4, 0), (5, 1)])
    level_3 = send(down_a, [(4, 0), (5, 1)])
    up_3 = send(up, [(1, 2), (2, 3)])
    return (down, wrap, level, down_a, down_b, up, level_2, level_3, up_3)


def dot_last(a, b):
    return lax.dot_general(a, b, (((1,), (1,)), ((), ())), preferred_element_type=F32)


def dot_first(a, b):
    return lax.dot_general(a, b, (((0,), (0,)), ((), ())), preferred_element_type=F32)


def dot(a, b):
    return jnp.dot(a, b, preferred_element_type=F32)


def mix_kernel(held, *refs):
    buffers, own, out_half, stacked, mixed = refs[:9], refs[9], refs[10], refs[11], refs[12]
    rank = own.shape[0]
    count = stacked.shape[0] // rank
    for r in range(1, count):
        rows = pl.ds((r - 1) * rank, rank)
        which = held[r - 1]

        @pl.when(which < 0)
        def _():
            stacked[rows, :] = jnp.zeros_like(own)

        for k in range(9):

            @pl.when(which == k)
            def _():
                stacked[rows, :] = buffers[k][...]

    stacked[pl.ds((count - 1) * rank, rank), :] = own[...]
    mixed[...] = dot_last(out_half[...], stacked[...])


def chain_kernel(*refs):
    tables, mixes = refs[:8], refs[8:15]
    hidden, factors, own_factor, cross = refs[15], refs[16], refs[17], refs[18]
    pairs = {8: jnp.zeros(tables[0].shape, BF)}
    later = jnp.zeros((tables[0].shape[0], 64), BF)
    found = {}
    for r in range(7, -1, -1):
        table = tables[r][...].astype(F32)
        total = table[:, :64]
        for p in range((8 - r) // 2):
            total = total + dot_last(pairs[r + 1 + 2 * p], mixes[r][:, p * LANES : (p + 1) * LANES])
        step = (total * table[:, 64:]).astype(BF)
        found[r] = step
        pairs[r] = jnp.concatenate([step, later], axis=1)
        later = step
    only_later = jnp.concatenate([pairs[1], pairs[3], pairs[5], pairs[7]], axis=1)
    factors[...] = jnp.concatenate(
        [pairs[1], pairs[3], pairs[5], jnp.concatenate([found[7], found[0]], axis=1)], axis=1
    )
    own_factor[...] = found[0]
    cross[...] = dot_first(hidden[...], only_later).astype(BF)


def grads_kernel(
    order, core, x, base, mine, theirs, own_factor, cross, kept, sent, packed, tall, wide
):
    step = pl.program_id(0)
    steps = pl.num_programs(0)
    half = steps // 2
    chunk = x.shape[3]
    tiles = chunk // LANES
    at = jnp.where(step < half, core[0], 1 - core[0]) * half + step % half
    tall[...] = dot_first(x[0].reshape(-1, chunk), own_factor[...])
    rows = chunk // 2
    low = tall[pl.ds(0, rows, stride=2), :]
    high = tall[pl.ds(1, rows, stride=2), :]
    packed[pl.ds(pl.multiple_of(at * rows, 8), rows), :] = jnp.concatenate([low, high], axis=1)

    @pl.when(step < half)
    def _():
        wide[...] = base[...] + dot(cross[...], mine[...])

    @pl.when(step >= half)
    def _():
        wide[...] = base[...] + dot(cross[...], theirs[...])

    per_row = tiles * steps
    half_rows = packed.shape[0] // 2
    for group in range(wide.shape[0] // 8):
        for tile in range(tiles):
            start = half_rows + group * 8 * per_row + at * tiles + tile
            packed[pl.ds(start, 8, stride=per_row), :] = wide[
                group * 8 : group * 8 + 8, tile * LANES : (tile + 1) * LANES
            ]

    @pl.when(step == steps - 1)
    def _():
        size = kept.shape[1]
        for i in range(kept.shape[0]):
            at_kept = pl.multiple_of(order[i] * size, 8)
            kept[i] = packed[pl.ds(at_kept, size), :].astype(BF)
            at_sent = pl.multiple_of(order[kept.shape[0] + i] * size, 8)
            sent[i] = packed[pl.ds(at_sent, size), :].astype(BF)


def out_kernel(plan, core, grads, mine, theirs, factors, out, work):
    step = pl.program_id(0)
    half = pl.num_programs(0) // 2
    count, rows, chunk = grads.shape

    def finish(block):
        moved = dot(factors[...], block[...])
        total = grads[...].reshape(-1, chunk).astype(F32) + moved
        work[...] = total.astype(BF).reshape(count, rows, chunk)

    @pl.when(step < half)
    def _():
        finish(mine)

    @pl.when(step >= half)
    def _():
        finish(theirs)

    for slot in range(count):
        out[0, slot] = work[plan[slot]]


def silu_slope(pre_value):
    gate_value = jax.nn.sigmoid(pre_value)
    return gate_value * (1.0 + pre_value * (1.0 - gate_value))


def whole(shape):
    return pl.BlockSpec(shape, lambda *_: (0,) * len(shape))


def reduced_block(kept, sent):
    got = send(sent, [(0, 1), (1, 0)], "dp_2")
    pair = (kept.astype(F32) + got.astype(F32)).reshape(4, 4, *kept.shape[1:])
    parts = [pair[k].astype(BF) for k in range(4)]
    total = pair[0]
    for k in (1, 2, 3):
        total = total + send(parts[k], [(i, (i + k) % 4) for i in range(4)], "dp_1").astype(F32)
    parts = [total[k].astype(BF) for k in range(4)]
    result = total[0]
    for k in (1, 2, 3):
        result = result + send(parts[k], [(i, (i + k) % 4) for i in range(4)], "dp_0").astype(F32)
    return result


def per_device(
    activations,
    loss_grads,
    adapter_in,
    adapter_out,
    first_moment,
    second_moment,
    old_owner,
    new_owner,
    plan,
):
    section = lax.axis_index("section")
    core = lax.axis_index("dp_2")
    replicas = lax.axis_size(DP)
    count, rows, width = loss_grads.shape
    rank = adapter_in.shape[2]
    tokens = count * rows
    half = width // 2
    owners_old = old_owner[0]
    owners_new = new_owner[0]
    block_len = first_moment.shape[2] // 2
    block_rows = block_len // LANES
    replica_ids = jnp.arange(replicas, dtype=jnp.int32)

    own_half = lax.dynamic_slice_in_dim(adapter_in[0], core * half, half, 0).T
    buffers = gather_later(own_half)

    flat_inputs = activations[0].reshape(tokens, width)
    flat_grads = loss_grads.reshape(tokens, width)
    pre_value = dot(flat_inputs, adapter_in[0])
    direct = dot(flat_grads, adapter_out[0].T)
    hidden = jax.nn.silu(pre_value).astype(BF)
    table = jnp.concatenate([direct.astype(BF), silu_slope(pre_value).astype(BF)], axis=1)
    base = dot(hidden.T, flat_grads)
    tables = [table] + [send(table, [(s, s - k) for s in range(k, 8)]) for k in range(1, 8)]

    owner_match = owners_new[None, :] == replica_ids[:, None]
    inverse = jnp.sum(jnp.where(owner_match, replica_ids[None, :], 0), axis=1)
    inverse = jnp.clip(inverse, 0, replicas - 1)
    my_z, my_y = lax.axis_index("dp_0"), lax.axis_index("dp_1")
    ys = (my_y + jnp.arange(4, dtype=jnp.int32))[:, None] % 4
    zs = (my_z + jnp.arange(4, dtype=jnp.int32))[None, :] % 4
    target = (zs * 8 + ys * 2).reshape(-1)
    targets = jnp.concatenate([target + core, target + 1 - core])
    match = targets[:, None] == replica_ids[None, :]
    order = jnp.sum(jnp.where(match, inverse[None, :], 0), axis=1).astype(jnp.int32)

    piece = PIECE_ROWS * LANES

    def pieces_of(moment):
        padded = jnp.pad(
            moment.reshape(2, block_len), ((0, 0), (0, replicas * piece - block_len))
        )
        return padded.reshape(2, replicas, piece)

    both = jnp.stack([pieces_of(first_moment[0, 0]), pieces_of(second_moment[0, 0])])
    spread = lax.all_to_all(
        both.transpose(2, 1, 0, 3).reshape(replicas, 4 * piece),
        DP,
        split_axis=0,
        concat_axis=0,
        tiled=True,
    )
    holder = jnp.sum(
        jnp.where(
            (inverse // 2)[:, None] == jnp.arange(owners_old.shape[0])[None, :],
            owners_old[None, :],
            0,
        ),
        axis=1,
    )
    wanted = jnp.clip(holder * 2 + inverse % 2, 0, 2 * replicas - 1)
    routed = jnp.take(spread.reshape(2 * replicas, 2 * piece), wanted, axis=0)
    arrived = lax.all_to_all(routed, DP, split_axis=0, concat_axis=0, tiled=True)
    arrived = arrived.reshape(replicas, 2, piece)
    first_old = arrived[:, 0].reshape(-1)[:block_len]
    second_old = arrived[:, 1].reshape(-1)[:block_len]

    held = jnp.asarray(HELD, jnp.int32)[section]
    out_half = lax.dynamic_slice_in_dim(adapter_out[0], core * half, half, 1)
    sections = len(HELD)
    vmem = pl.BlockSpec(memory_space=pltpu.VMEM)
    stacked, mixed = pl.pallas_call(
        mix_kernel,
        out_shape=(
            jax.ShapeDtypeStruct((sections * rank, half), BF),
            jax.ShapeDtypeStruct((rank, sections * rank), F32),
        ),
        in_specs=[pl.BlockSpec(memory_space=pltpu.SMEM)] + [vmem] * 11,
        out_specs=(vmem, vmem),
        cost_estimate=pl.CostEstimate(
            flops=2 * sections * rank * rank * half, bytes_accessed=8_000_000, transcendentals=0
        ),
        name="mix",
    )(held, *buffers, own_half, out_half)
    swap = [(0, 1), (1, 0)]
    mixed = (mixed + send(mixed, swap, "dp_2")).astype(BF)
    theirs = send(stacked, swap, "dp_2")
    mixes = [mixed]
    for k in range(1, 7):
        wide = (8 - k) // 2 * LANES
        mixes.append(send(mixed[:, :wide], [(s, s - k) for s in range(k, 8)]))

    factors, own_factor, cross = pl.pallas_call(
        chain_kernel,
        out_shape=(
            jax.ShapeDtypeStruct((tokens, sections * rank), BF),
            jax.ShapeDtypeStruct((tokens, rank), BF),
            jax.ShapeDtypeStruct((rank, sections * rank), BF),
        ),
        in_specs=[vmem] * 16,
        out_specs=(vmem,) * 3,
        name="chain",
    )(*tables, *mixes, hidden)

    steps = 6
    chunk = width // steps
    core_word = core.astype(jnp.int32).reshape(1)

    def at_of(step, core_ref):
        near = step < steps // 2
        return jnp.where(near, core_ref[0], 1 - core_ref[0]) * (steps // 2) + step % (steps // 2)

    mine_spec = pl.BlockSpec(
        (sections * rank, chunk), lambda i, *_: (0, jnp.minimum(i, steps // 2 - 1))
    )
    theirs_spec = pl.BlockSpec(
        (sections * rank, chunk), lambda i, *_: (0, jnp.maximum(i - steps // 2, 0))
    )
    kept, sent = pl.pallas_call(
        grads_kernel,
        grid_spec=pltpu.PrefetchScalarGridSpec(
            num_scalar_prefetch=2,
            grid=(steps,),
            in_specs=[
                pl.BlockSpec((1, count, rows, chunk), lambda i, o, c: (0, 0, 0, at_of(i, c))),
                pl.BlockSpec((rank, chunk), lambda i, o, c: (0, at_of(i, c))),
                mine_spec,
                theirs_spec,
                whole((tokens, rank)),
                whole((rank, sections * rank)),
            ],
            out_specs=(
                whole((replicas // 2, block_rows, LANES)),
                whole((replicas // 2, block_rows, LANES)),
            ),
            scratch_shapes=[
                pltpu.VMEM((replicas * block_rows, LANES), F32),
                pltpu.VMEM((chunk, rank), F32),
                pltpu.VMEM((rank, chunk), F32),
            ],
        ),
        out_shape=(
            jax.ShapeDtypeStruct((replicas // 2, block_rows, LANES), BF),
            jax.ShapeDtypeStruct((replicas // 2, block_rows, LANES), BF),
        ),
        name="grads",
    )(order, core_word, activations, base, stacked, theirs, own_factor, cross)

    emitted = pl.pallas_call(
        out_kernel,
        grid_spec=pltpu.PrefetchScalarGridSpec(
            num_scalar_prefetch=2,
            grid=(steps,),
            in_specs=[
                pl.BlockSpec((count, rows, chunk), lambda i, o, c: (0, 0, at_of(i, c))),
                mine_spec,
                theirs_spec,
                whole((tokens, sections * rank)),
            ],
            out_specs=pl.BlockSpec((1, count, rows, chunk), lambda i, o, c: (0, 0, 0, at_of(i, c))),
            scratch_shapes=[pltpu.VMEM((count, rows, chunk), BF)],
        ),
        out_shape=jax.ShapeDtypeStruct((1, count, rows, width), BF),
        cost_estimate=pl.CostEstimate(
            flops=2 * tokens * sections * rank * width,
            bytes_accessed=2 * tokens * width * 2,
            transcendentals=0,
        ),
        name="emit",
    )(plan, core_word, loss_grads, stacked, theirs, factors)

    grads = reduced_block(kept, sent).reshape(-1) / loss_scale
    first_next = beta_one * first_old + (1.0 - beta_one) * grads
    second_next = beta_two * second_old + (1.0 - beta_two) * grads * grads
    update = (
        first_next
        / (1.0 - beta_one**adam_step)
        / (jnp.sqrt(second_next / (1.0 - beta_two**adam_step)) + adam_eps)
    )
    return (emitted, update[None, None], first_next[None, None], second_next[None, None])


def solution(mesh):
    torus = Mesh(
        mesh.devices.reshape(mesh.shape["section"], 4, 4, 2), ("section", "dp_0", "dp_1", "dp_2")
    )
    in_specs = (
        P("section", None, DP, None),
        P(None, DP, None),
        P("section", None, None),
        P("section", None, None),
        P("section", DP, None),
        P("section", DP, None),
        P("section", None),
        P("section", None),
        P(),
    )
    out_specs = (
        P("section", None, DP, None),
        P("section", DP, None),
        P("section", DP, None),
        P("section", DP, None),
    )
    return jax.shard_map(
        per_device, mesh=torus, in_specs=in_specs, out_specs=out_specs, check_vma=False
    )
```
